32 devices in a mesh: row: 2 (over y), col: 4 (over z), depth: 4 (over x, core).
Axes of the slice: x: 2, y: 2, z: 4, core: 2. Of those that a mesh axis runs over, the one named last changes fastest.
Arguments:
- grad_out: bfloat16 [1024, 6144], P('depth', 'col'), may hold values from -6 to 6
- pre_act: bfloat16 [1024, 24576], P('depth', 'row'), may hold values from -8 to 8
- down_weight: bfloat16 [24576, 6144], P(('row', 'depth'), 'col'), may hold values from -0.0546875 to 0.0546875
Outputs:
- grad_pre: bfloat16 [1024, 24576], P('depth', 'row')
- grad_weight: bfloat16 [24576, 6144], P(('row', 'depth'), 'col')
The draws below stay inside these ranges and needn't reach their ends.
All inputs are finite; a program needn't handle non-finite values.
Results may differ from the reference program's by a relative error of at most 0.0066.
Values may be sent and summed in bfloat16 or wider, within the bound.
No kernel may reach another device: no remote copies, remote signals or barrier semaphores. Data moves between devices by JAX's collectives and lax.ppermute only.
A program may use at most 128 MiB of HBM per device.

```python
import jax
import jax.numpy as jnp

D = 6144
FF = 24576
TOKENS = 1024


def with_spikes(values, rng, source, target, shards_of, factor):
    owner, partner = [(jnp.arange(values.shape[dim]) // (values.shape[dim] // shards_of)).reshape([-1 if axis == dim else 1 for axis in range(values.ndim)]) for dim in (source, target)]
    chosen = jax.random.permutation(rng, shards_of)[partner]
    strong = (owner == chosen) | (owner == (partner + shards_of // 2) % shards_of)
    return jnp.where(strong, factor * values, values)


def levels(stream_key, extent, cuts, low, largest):
    gain, own = 1.0, jax.random.fold_in(stream_key, 6)
    for position, parts in cuts:
        heights = jnp.exp(jax.random.uniform(jax.random.fold_in(own, position), (parts,), jnp.float32, low / len(cuts), largest / len(cuts)))
        gain = gain * jnp.repeat(heights, extent[position] // parts).reshape([-1 if axis == position else 1 for axis in range(len(extent))])
    return gain


def scatter_about(stream_key, dims, spread, bound, shards=(), held_as=jnp.bfloat16):
    entries = spread * jax.random.normal(stream_key, dims, jnp.float32)
    if shards:
        entries = entries * levels(stream_key, dims, shards, -0.22, 0.18)
    return jnp.clip(entries, -bound, bound).astype(held_as)


def gaussian_with(key, dims, spread, reach, pieces, heavy, held_as=jnp.bfloat16):
    drawn = spread * jax.random.normal(key, dims, jnp.float32)
    if pieces:
        drawn = drawn * levels(key, dims, pieces, -0.22, 0.18)
    return jnp.clip(with_spikes(drawn, jax.random.fold_in(key, 3), *heavy), -reach, reach).astype(held_as)


def setup_inputs(seed: int = 0) -> dict:
    arg_keys = jax.random.split(jax.random.key(seed), 4)
    grad_out = scatter_about(arg_keys[0], (TOKENS, D), 1.0, 6.0, ((0, 4), (1, 4)))
    pre_act = gaussian_with(arg_keys[1], (TOKENS, FF), 1.5, 8.0, ((0, 4), (1, 2)), (0, 1, 4, 2.0))
    down_weight = gaussian_with(arg_keys[2], (FF, D), FF ** -0.5, 0.0546875, ((0, 8), (1, 4)), (1, 0, 8, 2.0))
    return dict(grad_out=grad_out, pre_act=pre_act, down_weight=down_weight)


sqrt_two_pi = 0.7978845608028654
cubic_coeff = 0.044715

def gelu_value(preact):
    tangent = jnp.tanh(sqrt_two_pi * (preact + cubic_coeff * preact * preact * preact))
    return 0.5 * preact * (1.0 + tangent)

def gelu_slope(preact):
    tangent = jnp.tanh(sqrt_two_pi * (preact + cubic_coeff * preact * preact * preact))
    inner = sqrt_two_pi * (1.0 + 3.0 * cubic_coeff * preact * preact)
    return 0.5 * (1.0 + tangent) + 0.5 * preact * (1.0 - tangent * tangent) * inner

def reference(grad_out, pre_act, down_weight):
    widened = pre_act.astype(jnp.float32)
    activation = gelu_value(widened).astype(jnp.bfloat16)
    backward = jnp.dot(grad_out, down_weight.T, preferred_element_type=jnp.float32)
    grad_pre = (backward * gelu_slope(widened)).astype(jnp.bfloat16)
    grad_weight = jnp.dot(activation.T, grad_out, preferred_element_type=jnp.float32).astype(jnp.bfloat16)
    return (grad_pre, grad_weight)
```

```python
import jax
import jax.numpy as jnp
from jax import lax
from jax.sharding import PartitionSpec as P

sqrt_two_pi = 0.7978845608028654
cubic_coeff = 0.044715
PARTS = 2
LAGS = (3, 4, 5)


def gelu_value(preact):
    tangent = jnp.tanh(sqrt_two_pi * (preact + cubic_coeff * preact * preact * preact))
    return 0.5 * preact * (1.0 + tangent)


def gelu_slope(preact):
    tangent = jnp.tanh(sqrt_two_pi * (preact + cubic_coeff * preact * preact * preact))
    inner = sqrt_two_pi * (1.0 + 3.0 * cubic_coeff * preact * preact)
    return 0.5 * (1.0 + tangent) + 0.5 * preact * (1.0 - tangent * tangent) * inner


def contract_last(left, right):
    return lax.dot_general(
        left, right, (((1,), (1,)), ((), ())), preferred_element_type=jnp.float32
    )


def contract_first(left, right):
    return lax.dot_general(
        left, right, (((0,), (0,)), ((), ())), preferred_element_type=jnp.float32
    )


def flip(value, offset, depth):
    if offset == 0:
        return value
    return lax.ppermute(value, "depth", [(d, d ^ offset) for d in range(depth)])


def reduce_piece(partial_value, offset, depth):
    tokens, width = partial_value.shape
    place = lax.axis_index("col")
    inner = (place == 1) | (place == 2)
    side = place // 2
    bf16 = jnp.bfloat16
    inward = lax.ppermute(partial_value.astype(bf16), "col", [(0, 1), (3, 2)])
    mine = partial_value.reshape(2, tokens // 2, width)
    inward = inward.reshape(2, tokens // 2, width)

    def half(which):
        own = lax.dynamic_index_in_dim(mine, which, 0, keepdims=False)
        other = lax.dynamic_index_in_dim(inward, which, 0, keepdims=False)
        return own + other.astype(jnp.float32)

    across = lax.ppermute(half(1 - side).astype(bf16), "col", [(1, 2), (2, 1)])
    total = (half(side) + across.astype(jnp.float32)).astype(bf16)
    if offset:
        pairs = [(c * depth + d, c * depth + (d ^ offset)) for c in (1, 2) for d in range(depth)]
        total = lax.ppermute(total, ("col", "depth"), pairs)
    outward_near = lax.ppermute(total, "col", [(1, 0), (2, 3)])
    other = lax.ppermute(total, "col", [(1, 2), (2, 1)])
    outward_far = lax.ppermute(other, "col", [(1, 0), (2, 3)])
    near = jnp.where(inner, total, outward_near)
    far = jnp.where(inner, other, outward_far)
    halves = jnp.where(side == 0, near, far), jnp.where(side == 0, far, near)
    return halves, (across, other, outward_far)


def plain_piece(partial_value, offset, depth):
    total = flip(lax.psum(partial_value, "col").astype(jnp.bfloat16), offset, depth)
    return tuple(jnp.split(total, 2, axis=0)), (total, total, total)


def make_on_device(cols, depth):
    piece = reduce_piece if cols == 4 else plain_piece
    order = [0] + list(range(2, depth)) + [1] if depth > 1 else [0]

    def on_device(grad_out, pre_act, down_weight):
        hidden = down_weight.shape[0]
        width = hidden // PARTS
        tokens = grad_out.shape[0]
        me = lax.axis_index("depth")
        grads = {k: flip(grad_out, k, depth) for k in order}
        pres = {}
        for k in order:
            block = lax.dynamic_slice_in_dim(pre_act, (me ^ k) * hidden, hidden, axis=1)
            pres[k] = flip(block, k, depth)
        stages = []
        grad_pre = jnp.zeros(pre_act.shape, jnp.bfloat16)
        for k in order:
            for part in range(PARTS):
                rows = down_weight[part * width : (part + 1) * width]
                behind = [
                    stages[len(stages) - lag][which]
                    for which, lag in enumerate(LAGS)
                    if len(stages) >= lag
                ]
                gated = lax.optimization_barrier((grads[k], *behind))[0]
                halves, marks = piece(contract_last(gated, rows), k, depth)
                stages.append(marks)
                start = (me ^ k) * hidden + part * width
                for i, back in enumerate(halves):
                    top = i * (tokens // 2)
                    saved = lax.dynamic_slice(pre_act, (top, start), (tokens // 2, width))
                    value = back.astype(jnp.float32) * gelu_slope(saved.astype(jnp.float32))
                    grad_pre = lax.dynamic_update_slice(
                        grad_pre, value.astype(jnp.bfloat16), (top, start)
                    )
        act = jnp.concatenate(
            [gelu_value(pres[k].astype(jnp.float32)).astype(jnp.bfloat16) for k in order], axis=0
        )
        every_grad = jnp.concatenate([grads[k] for k in order], axis=0)
        grad_weight = contract_first(act, every_grad).astype(jnp.bfloat16)
        return (grad_pre, grad_weight)

    return on_device


def solution(mesh):
    placed = (P("depth", "col"), P("depth", "row"), P(("row", "depth"), "col"))
    return jax.shard_map(
        make_on_device(mesh.shape["col"], mesh.shape["depth"]),
        mesh=mesh,
        in_specs=placed,
        out_specs=(P("depth", "row"), P(("row", "depth"), "col")),
        check_vma=False,
    )
```
